32 devices in a mesh: col: 4 (over z), row: 8 (over y, x, core).
Axes of the slice: x: 2, y: 2, z: 4, core: 2. Of those that a mesh axis runs over, the one named last changes fastest.
Arguments:
- trans_mat: bfloat16 [24576, 24576], P('row', 'col')
- x_start: float32 [24576, 256], P(('col', 'row'))
- teleport: float32 [24576, 256], P(('col', 'row'))
- dangling: int32 [24576], P(('col', 'row'))
Outputs:
- output: float32 [24576, 256], P(('col', 'row'))
All inputs are finite; a program needn't handle non-finite values.
Results may differ from the reference program's by a relative error of at most 0.001.
Values are sent between devices in bfloat16 or wider.
A program may use at most 1 GiB of HBM per device.

```python
import jax
import jax.numpy as jnp
from jax import lax

VERTICES = 24576
VECS = 256
DEGREE = 6
SWEEPS = 8
DAMPING = 0.85


def draw_graph(key_dang, key_target, key_edge):
    dangling = (jax.random.randint(key_dang, (VERTICES,), 0, 5) == 0).astype(jnp.int32)
    live_cols = (1 - dangling).astype(jnp.bfloat16)
    target = jax.random.randint(key_target, (VERTICES,), 0, VERTICES)
    row_blocks = 16
    block_rows = VERTICES // row_blocks
    block_keys = jax.random.split(key_edge, row_blocks)
    block_starts = jnp.arange(row_blocks, dtype=jnp.int32) * block_rows

    def edge_block(block_args):
        block_key, block_start = block_args
        draw_vals = jax.random.randint(block_key, (block_rows, VERTICES), 0, VERTICES)
        row_ids = block_start + jnp.arange(block_rows, dtype=jnp.int32)[:, None]
        edge_mask = (draw_vals < DEGREE) | (row_ids == target[None, :])
        return edge_mask.astype(jnp.bfloat16) * live_cols[None, :]

    adjacency = lax.map(edge_block, (block_keys, block_starts)).reshape(VERTICES, VERTICES)
    out_degree = jnp.sum(adjacency, axis=0, dtype=jnp.float32)
    inv_degree = (1.0 / jnp.maximum(out_degree, 1.0)).astype(jnp.bfloat16)
    trans_mat = adjacency * inv_degree[None, :]
    return trans_mat, dangling


def setup_inputs(seed: int = 0) -> dict:
    base_key = jax.random.key(seed)
    k_dang, k_target, k_edge, k_start, k_scale, k_center, k_weight = jax.random.split(base_key, 7)
    trans_mat, dangling = draw_graph(k_dang, k_target, k_edge)
    col_scale = 2.0 ** jax.random.uniform(k_scale, (1, VECS), jnp.float32, -2.0, 2.0)
    x_start = jax.random.uniform(k_start, (VERTICES, VECS), jnp.float32, 0.0, 2.0) * col_scale
    centers = jax.random.randint(k_center, (1, VECS), 0, VERTICES)
    offsets = (jnp.arange(VERTICES, dtype=jnp.int32)[:, None] - centers) % VERTICES
    inside = (offsets < VERTICES // 8).astype(jnp.float32)
    raw_tele = inside * jax.random.uniform(k_weight, (VERTICES, VECS), jnp.float32, 0.5, 2.0)
    teleport = raw_tele * (VERTICES / jnp.sum(raw_tele, axis=0, keepdims=True))
    return {'trans_mat': trans_mat, 'x_start': x_start, 'teleport': teleport, 'dangling': dangling}


def reference(trans_mat, x_start, teleport, dangling):
    dang_col = dangling.astype(jnp.float32)[:, None]

    def one_sweep(x_cur, unused):
        dang_mass = jnp.sum(dang_col * x_cur, axis=0) / VERTICES
        spread = jnp.dot(trans_mat, x_cur.astype(jnp.bfloat16), preferred_element_type=jnp.float32)
        x_next = DAMPING * spread + (DAMPING * dang_mass + (1.0 - DAMPING))[None, :] * teleport
        return x_next, None

    x_final, unused_out = lax.scan(one_sweep, x_start, None, length=SWEEPS)
    return x_final
```

```python
import functools

import jax
import jax.numpy as jnp
from jax import lax
from jax.experimental import pallas as pl
from jax.experimental.pallas import tpu as pltpu
from jax.sharding import PartitionSpec as P

SWEEPS = 8
DAMPING = 0.85
MESH = pl.DeviceIdType.MESH

CHUNKS = 8
PERIOD = 8
HOP = 2
GATHER = 2
FORWARD = 3
READY = 3
RING = 4
PASSES = 2 * SWEEPS


def kernel(block_rows, lanes, a_hbm, x_ref, v_ref, d_ref, out_ref,
           a_v, xbuf, rbuf, sums, xs, vbuf, dbuf, sacc, sstage, sbuf, coef,
           a_sem, r_send, r_recv, z_send, z_recv, g_send, g_recv, f_send, f_recv,
           s_send, s_recv, v_send, v_recv, d_send, d_recv, x0_send, x0_recv, x1_send, x1_recv, o_recv):
    z = lax.axis_index('col')
    row = lax.axis_index('row')
    k = row % 2
    x = (row // 2) % 2
    y = row // 4
    c = row // 2
    half = block_rows // 2
    ch = half // CHUNKS
    sub = ch // 4
    piece = block_rows // 4
    vertices = block_rows * 8
    inplane = (y * 4 + (1 - x) * 2 + k, (1 - y) * 4 + x * 2 + k, (1 - y) * 4 + (1 - x) * 2 + k)
    partner = c * 2 + (1 - k)

    def remote(src, dst, send, recv, dev):
        return pltpu.make_async_remote_copy(src_ref=src, dst_ref=dst, send_sem=send, recv_sem=recv,
                                            device_id=dev, device_id_type=MESH)

    def a_copy(dirn, q):
        rows = pl.ds(dirn * half + q * ch, ch)
        return pltpu.make_async_copy(a_hbm.at[rows], a_v.at[rows], a_sem.at[dirn, q])

    def start_a(q, carry):
        for dirn in range(2):
            a_copy(dirn, q).start()
        return carry
    lax.fori_loop(0, CHUNKS, start_a, 0)

    barrier = pltpu.get_barrier_semaphore()
    me = z * 8 + row

    def greet(step, carry):
        other = (me + step) % 32
        pl.semaphore_signal(barrier, inc=1, device_id=(other // 8, other % 8), device_id_type=MESH)
        return carry
    lax.fori_loop(1, 32, greet, 0)
    pl.semaphore_wait(barrier, 31)

    def x_rows(h, par, start, size):
        return xbuf.at[h, par, pl.ds(start, size)]

    def x0_copy(h, m):
        dev = inplane[m] if m < 3 else partner
        mine = x_rows(h, 0, row * piece, piece)
        return remote(mine, mine, x0_send.at[h, m], x0_recv.at[h, m], (z, dev))

    def x1_copy(h, m):
        theirs = x_rows(h, 0, inplane[m] * piece, piece)
        return remote(theirs, theirs, x1_send.at[h, m], x1_recv.at[h, m], (z, partner))

    for h in range(2):
        xbuf[h, 0, pl.ds(row * piece, piece), :] = x_ref[:, h * lanes:(h + 1) * lanes].astype(jnp.bfloat16)
        for m in range(4):
            x0_copy(h, m).start()

    def s_copy(h, holder):
        dev = (holder // 2, (holder // 2) * 2 + holder % 2)
        return remote(sstage.at[h], sbuf.at[h, me], s_send.at[h, holder], s_recv.at[h, me], dev)

    holds_v = c == z

    def s_start(h):
        for holder in range(8):
            mine = (holder // 2 == z) & ((holder // 2) * 2 + holder % 2 == row)

            @pl.when(mine)
            def _():
                sbuf[h, me] = sstage[h]

            @pl.when(jnp.logical_not(mine))
            def _():
                s_copy(h, holder).start()

    def s_wait_send(h):
        for holder in range(8):
            @pl.when(jnp.logical_not((holder // 2 == z) & ((holder // 2) * 2 + holder % 2 == row)))
            def _():
                s_copy(h, holder).wait_send()

    for h in range(2):
        terms = d_ref[...].astype(jnp.float32) * x_ref[:, h * lanes:(h + 1) * lanes]
        sstage[h] = jnp.sum(terms.reshape(piece // 8, 8, lanes), axis=0)
        s_start(h)

    v_dev = z * 2 + row // 4
    v_self = v_dev == row

    def v_copy(h):
        return remote(v_ref.at[:, pl.ds(h * lanes, lanes)], vbuf.at[h, pl.ds((row % 4) * piece, piece)],
                      v_send.at[h], v_recv.at[h, row % 4], (z, v_dev))

    @pl.when(v_self)
    def _():
        for h in range(2):
            vbuf[h, pl.ds((row % 4) * piece, piece), :] = v_ref[:, h * lanes:(h + 1) * lanes]

    d_plane = ((row % 4) // 2) * 3
    d_self = v_self & (d_plane == z)
    d_copy = remote(d_ref, dbuf.at[pl.ds((row % 2) * piece, piece)], d_send, d_recv.at[row % 2], (d_plane, v_dev))

    @pl.when(d_self)
    def _():
        dbuf[pl.ds((row % 2) * piece, piece), :] = d_ref[...]

    @pl.when(jnp.logical_not(v_self))
    def _():
        for h in range(2):
            v_copy(h).start()

    @pl.when(jnp.logical_not(d_self))
    def _():
        d_copy.start()

    for h in range(2):
        for m in range(3):
            x0_copy(h, m).wait_recv()
            x1_copy(h, m).start()
    for h in range(2):
        x0_copy(h, 3).wait_recv()
        for m in range(3):
            x1_copy(h, m).wait_recv()
        for m in range(4):
            x0_copy(h, m).wait_send()
        for m in range(3):
            x1_copy(h, m).wait_send()

    def index(step):
        n = step // PERIOD
        q = step % PERIOD
        valid = (step >= 0) & (n < PASSES) & (q < CHUNKS)
        return valid, n, q, n % 2, (n // 2) % 2

    def owner_is_reader(dirn):
        return (z == c) & (z == 3 * dirn)

    def slot(t, carry):
        def gather_copy(h, par, dirn, q, ring, m):
            rows = x_rows(h, 1 - par, k * block_rows + dirn * half + q * ch + c * sub, sub)
            return remote(rows, rows, g_send.at[ring, dirn, m], g_recv.at[h, dirn, q, m], (z, inplane[m]))

        def forward_copy(h, par, dirn, q, ring):
            rows = x_rows(h, 1 - par, k * block_rows + dirn * half + q * ch, ch)
            return remote(rows, rows, f_send.at[ring, dirn], f_recv.at[h, dirn, q], (z, partner))

        def forward(dirn):
            step = t - 3 * HOP - FORWARD
            old, n, q, h, par = index(step - RING)

            @pl.when(old & (n < PASSES - 2))
            def _():
                forward_copy(h, par, dirn, q, (step - RING) % RING).wait_send()
            valid, n, q, h, par = index(step)

            @pl.when(valid & (n < PASSES - 2))
            def _():
                for m in range(3):
                    gather_copy(h, par, dirn, q, step % RING, m).wait_recv()
                forward_copy(h, par, dirn, q, step % RING).start()

        def ready(dirn):
            step = t - 3 * HOP - READY
            valid, n, q, h, par = index(step)

            @pl.when(valid & (n < PASSES - 2))
            def _():
                forward_copy(h, par, dirn, q, step % RING).wait_recv()

        def gather(dirn):
            step = t - 3 * HOP - GATHER
            old, n, q, h, par = index(step - RING)

            @pl.when(old & (n < PASSES - 2))
            def _():
                for m in range(3):
                    gather_copy(h, par, dirn, q, (step - RING) % RING, m).wait_send()
            valid, n, q, h, par = index(step)

            @pl.when(valid & (n < PASSES - 2))
            def _():
                @pl.when(jnp.logical_not(owner_is_reader(dirn)))
                def _():
                    rows = x_rows(h, 1 - par, k * block_rows + dirn * half + q * ch + c * sub, sub)
                    remote(rows, rows, z_send.at[0, 0], z_recv.at[h, dirn, q], (z, row)).wait_recv()
                for m in range(3):
                    gather_copy(h, par, dirn, q, step % RING, m).start()

        def dangling_term():
            near = jnp.minimum(z, 3 - z)
            step = t - HOP * near
            valid, n, q, h, par = index(step)

            @pl.when(holds_v & valid & (q == 0))
            def _():
                def wait_one(src, carry):
                    sends = ((n < 2) | (src // 8 == 0) | (src // 8 == 3)) & (src != me)

                    @pl.when(sends)
                    def _():
                        remote(sstage.at[h], sbuf.at[h, src], s_send.at[h, 0], s_recv.at[h, src], (z, row)).wait_recv()
                    return carry
                lax.fori_loop(0, 32, wait_one, 0)

                @pl.when(n < 2)
                def _():
                    for piece_idx in range(4):
                        @pl.when(4 * k + piece_idx != row)
                        def _():
                            rows = vbuf.at[h, pl.ds(piece_idx * piece, piece)]
                            remote(rows, rows, v_send.at[0], v_recv.at[h, piece_idx], (z, row)).wait_recv()
                ends = jnp.sum(sbuf[h, 0:8], axis=0) + jnp.sum(sbuf[h, 24:32], axis=0)
                coef[h] = ends

                @pl.when(n < 2)
                def _():
                    coef[h] += jnp.sum(sbuf[h, 8:24], axis=0)
                mass = jnp.sum(coef[h], axis=0, keepdims=True) / vertices
                coef[h] = jnp.broadcast_to(DAMPING * mass + (1.0 - DAMPING), (8, lanes))

        def reduce(dirn):
            pos = z if dirn == 1 else 3 - z
            after = z + 1 if dirn == 1 else z - 1
            owner = pos == 3

            def sum_copy(h, q, ring):
                return remote(sums.at[dirn, ring], rbuf.at[dirn, h, q], r_send.at[dirn, ring], r_recv.at[dirn, h, q],
                              (after, row))

            def out_place(h, q):
                rows = pl.ds((q % 4) * ch, ch)
                return out_ref.at[rows, pl.ds(pl.multiple_of(h * lanes, lanes), lanes)]

            def out_row(q):
                return 4 * k + 2 * dirn + q // 4

            def out_here(q):
                return (z == c) & (out_row(q) == row)

            def out_copy(h, q, ring):
                return remote(sums.at[dirn, ring], out_place(h, q), r_send.at[dirn, ring], o_recv.at[h, q % 4],
                              (c, out_row(q)))

            def share_copy(h, par, q, ring, cc):
                rows = x_rows(h, 1 - par, k * block_rows + dirn * half + q * ch + cc * sub, sub)
                return remote(xs.at[ring, pl.ds(cc * sub, sub)], rows, z_send.at[ring, cc], z_recv.at[h, dirn, q],
                              (c, 2 * cc + k))

            step = t - HOP * pos
            old, n, q, h, par = index(step - RING)
            ring = (step - RING) % RING

            @pl.when(old & jnp.logical_not(owner))
            def _():
                sum_copy(h, q, ring).wait_send()

            @pl.when(old & owner & (n < PASSES - 2))
            def _():
                for cc in range(4):
                    @pl.when(jnp.logical_not((z == c) & (cc == c)))
                    def _():
                        share_copy(h, par, q, ring, cc).wait_send()

                @pl.when(q == CHUNKS - 1)
                def _():
                    s_wait_send(h)

            @pl.when(old & owner & (n >= PASSES - 2) & jnp.logical_not(out_here(q)))
            def _():
                out_copy(h, q, ring).wait_send()

            valid, n, q, h, par = index(step)
            ring = step % RING

            @pl.when(valid)
            def _():
                start = dirn * half + q * ch
                rows = pl.ds(start, ch)

                @pl.when(n == 0)
                def _():
                    a_copy(dirn, q).wait()
                prod = jnp.dot(a_v[rows, :], xbuf[h, par], preferred_element_type=jnp.float32)
                sums[dirn, ring] = prod * DAMPING

                @pl.when(holds_v)
                def _():
                    sums[dirn, ring] += coef[h, 0:1, :] * vbuf[h, rows, :]

                @pl.when(pos > 0)
                def _():
                    sum_copy(h, q, ring).wait_recv()
                    sums[dirn, ring] += rbuf[dirn, h, q]

                @pl.when(jnp.logical_not(owner))
                def _():
                    sum_copy(h, q, ring).start()

                @pl.when(owner & (n < PASSES - 2))
                def _():
                    @pl.when((n == 0) & (q == 0))
                    def _():
                        for part in range(2):
                            @pl.when(jnp.logical_not((z == c) & (4 * k + 2 * dirn + part == row)))
                            def _():
                                place = dbuf.at[pl.ds(part * piece, piece)]
                                remote(d_ref, place, d_send, d_recv.at[part], (z, row)).wait_recv()
                    total = sums[dirn, ring]
                    low = total.astype(jnp.bfloat16)
                    xs[ring] = low
                    terms = dbuf[pl.ds(q * ch, ch), :].astype(jnp.float32) * total
                    mass = jnp.sum(terms.reshape(ch // 8, 8, lanes), axis=0)
                    for cc in range(4):
                        here = (z == c) & (cc == c)

                        @pl.when(here)
                        def _():
                            place = pl.ds(k * block_rows + start + cc * sub, sub)
                            xbuf[h, 1 - par, place, :] = low[cc * sub:(cc + 1) * sub]

                        @pl.when(jnp.logical_not(here))
                        def _():
                            share_copy(h, par, q, ring, cc).start()

                    @pl.when(q == 0)
                    def _():
                        sacc[...] = mass

                    @pl.when(q > 0)
                    def _():
                        sacc[...] += mass

                    @pl.when(q == CHUNKS - 1)
                    def _():
                        sstage[h] = sacc[...]
                        s_start(h)

                @pl.when(owner & (n >= PASSES - 2))
                def _():
                    @pl.when(out_here(q))
                    def _():
                        out_ref[pl.ds((q % 4) * ch, ch), pl.ds(pl.multiple_of(h * lanes, lanes), lanes)] = sums[dirn, ring]

                    @pl.when(jnp.logical_not(out_here(q)))
                    def _():
                        out_copy(h, q, ring).start()

        @pl.when(t == 1)
        def _():
            for h in range(2):
                s_wait_send(h)

            @pl.when(jnp.logical_not(v_self))
            def _():
                for h in range(2):
                    v_copy(h).wait_send()

            @pl.when(jnp.logical_not(d_self))
            def _():
                d_copy.wait_send()

        for dirn in range(2):
            forward(dirn)
        for dirn in range(2):
            ready(dirn)
        dangling_term()
        reduce(1)
        for dirn in range(2):
            gather(dirn)
        reduce(0)
        return carry

    lax.fori_loop(0, PASSES * PERIOD + 3 * HOP + FORWARD + RING, slot, 0)

    made_here = (z == 3 * ((row % 4) // 2)) & (row == 2 * z + row // 4)

    @pl.when(jnp.logical_not(made_here))
    def _():
        for h in range(2):
            for q in range(4):
                place = out_ref.at[pl.ds(q * ch, ch), pl.ds(h * lanes, lanes)]
                remote(place, place, d_send, o_recv.at[h, q], (z, row)).wait_recv()


def solution(mesh):
    def local_sweeps(mat_tile, x_piece, tele_piece, dang_piece):
        block_rows, src = mat_tile.shape
        piece, vecs = x_piece.shape
        lanes = vecs // 2
        ch = block_rows // 2 // CHUNKS
        dang = jnp.broadcast_to(dang_piece.astype(jnp.bfloat16)[:, None], (piece, lanes))
        dma = pltpu.SemaphoreType.DMA
        return pl.pallas_call(
            functools.partial(kernel, block_rows, lanes),
            name='sweeps',
            out_shape=jax.ShapeDtypeStruct((piece, vecs), jnp.float32),
            in_specs=[pl.BlockSpec(memory_space=pltpu.HBM)] + [pl.BlockSpec(memory_space=pltpu.VMEM)] * 3,
            out_specs=pl.BlockSpec(memory_space=pltpu.VMEM),
            scratch_shapes=[
                pltpu.VMEM((block_rows, src), jnp.bfloat16),
                pltpu.VMEM((2, 2, src, lanes), jnp.bfloat16),
                pltpu.VMEM((2, 2, CHUNKS, ch, lanes), jnp.float32),
                pltpu.VMEM((2, RING, ch, lanes), jnp.float32),
                pltpu.VMEM((RING, ch, lanes), jnp.bfloat16),
                pltpu.VMEM((2, block_rows, lanes), jnp.float32),
                pltpu.VMEM((block_rows // 2, lanes), jnp.bfloat16),
                pltpu.VMEM((8, lanes), jnp.float32),
                pltpu.VMEM((2, 8, lanes), jnp.float32),
                pltpu.VMEM((2, 32, 8, lanes), jnp.float32),
                pltpu.VMEM((2, 8, lanes), jnp.float32),
                dma((2, CHUNKS)),
                dma((2, RING)),
                dma((2, 2, CHUNKS)),
                dma((RING, 4)),
                dma((2, 2, CHUNKS)),
                dma((RING, 2, 3)),
                dma((2, 2, CHUNKS, 3)),
                dma((RING, 2)),
                dma((2, 2, CHUNKS)),
                dma((2, 8)),
                dma((2, 32)),
                dma((2,)),
                dma((2, 4)),
                dma,
                dma((2,)),
                dma((2, 4)),
                dma((2, 4)),
                dma((2, 3)),
                dma((2, 3)),
                dma((2, 4)),
            ],
            compiler_params=pltpu.CompilerParams(collective_id=0, has_side_effects=True,
                                                 vmem_limit_bytes=64 * 1024 * 1024 - 65536),
        )(mat_tile, x_piece, tele_piece, dang)

    vec_spec = P(('col', 'row'), None)
    return jax.shard_map(local_sweeps, mesh=mesh,
                         in_specs=(P('row', 'col'), vec_spec, vec_spec, P(('col', 'row'))),
                         out_specs=vec_spec, check_vma=False)
```

```python
import functools

import jax
import jax.numpy as jnp
from jax import lax
from jax.experimental import pallas as pl
from jax.experimental.pallas import tpu as pltpu
from jax.sharding import PartitionSpec as P

SWEEPS = 8
DAMPING = 0.85
MESH = pl.DeviceIdType.MESH

CHUNKS = 12
PERIOD = 12
HOP = 2
GATHER = 4
FORWARD = 6
READY = 7
RING = 4
PASSES = 2 * SWEEPS


def kernel(block_rows, lanes, a_hbm, x_ref, v_ref, d_ref, out_ref,
           a_v, xbuf, rbuf, sums, xs, vbuf, dbuf, sacc, sstage, sbuf, coef,
           a_sem, r_send, r_recv, z_send, z_recv, g_send, g_recv, f_send, f_recv,
           s_send, s_recv, v_send, v_recv, d_send, d_recv, x0_send, x0_recv, x1_send, x1_recv, o_recv):
    z = lax.axis_index('col')
    row = lax.axis_index('row')
    k = row % 2
    x = (row // 2) % 2
    y = row // 4
    c = row // 2
    half = block_rows // 2
    ch = half // CHUNKS
    sub = ch // 4
    piece = block_rows // 4
    vertices = block_rows * 8
    inplane = (y * 4 + (1 - x) * 2 + k, (1 - y) * 4 + x * 2 + k, (1 - y) * 4 + (1 - x) * 2 + k)
    partner = c * 2 + (1 - k)

    def remote(src, dst, send, recv, dev):
        return pltpu.make_async_remote_copy(src_ref=src, dst_ref=dst, send_sem=send, recv_sem=recv,
                                            device_id=dev, device_id_type=MESH)

    def a_copy(dirn, q):
        rows = pl.ds(dirn * half + q * ch, ch)
        return pltpu.make_async_copy(a_hbm.at[rows], a_v.at[rows], a_sem.at[dirn, q])

    def start_a(q, carry):
        for dirn in range(2):
            a_copy(dirn, q).start()
        return carry
    lax.fori_loop(0, CHUNKS, start_a, 0)

    for h in range(2):
        xbuf[h, 0, pl.ds(row * piece, piece), :] = x_ref[:, h * lanes:(h + 1) * lanes].astype(jnp.bfloat16)
        terms = d_ref[...].astype(jnp.float32) * x_ref[:, h * lanes:(h + 1) * lanes]
        sstage[h] = jnp.sum(terms.reshape(piece // 8, 8, lanes), axis=0)

    barrier = pltpu.get_barrier_semaphore()
    me = z * 8 + row

    def greet(step, carry):
        other = (me + step) % 32
        pl.semaphore_signal(barrier, inc=1, device_id=(other // 8, other % 8), device_id_type=MESH)
        return carry
    lax.fori_loop(1, 32, greet, 0)
    pl.semaphore_wait(barrier, 31)

    def x_rows(h, par, start, size):
        return xbuf.at[h, par, pl.ds(start, size)]

    def x0_copy(h, m):
        dev = inplane[m] if m < 3 else partner
        mine = x_rows(h, 0, row * piece, piece)
        return remote(mine, mine, x0_send.at[h, m], x0_recv.at[h, m], (z, dev))

    def x1_copy(h, m):
        theirs = x_rows(h, 0, inplane[m] * piece, piece)
        return remote(theirs, theirs, x1_send.at[h, m], x1_recv.at[h, m], (z, partner))


    def s_copy(h, holder):
        dev = (holder // 2, (holder // 2) * 2 + holder % 2)
        return remote(sstage.at[h], sbuf.at[h, me], s_send.at[h, holder], s_recv.at[h, me], dev)

    holds_v = c == z

    def s_start(h):
        for holder in range(8):
            mine = (holder // 2 == z) & ((holder // 2) * 2 + holder % 2 == row)

            @pl.when(mine)
            def _():
                sbuf[h, me] = sstage[h]

            @pl.when(jnp.logical_not(mine))
            def _():
                s_copy(h, holder).start()

    def s_wait_send(h):
        for holder in range(8):
            @pl.when(jnp.logical_not((holder // 2 == z) & ((holder // 2) * 2 + holder % 2 == row)))
            def _():
                s_copy(h, holder).wait_send()


    v_dev = z * 2 + row // 4
    v_self = v_dev == row

    def v_copy(h):
        return remote(v_ref.at[:, pl.ds(h * lanes, lanes)], vbuf.at[h, pl.ds((row % 4) * piece, piece)],
                      v_send.at[h], v_recv.at[h, row % 4], (z, v_dev))

    @pl.when(v_self)
    def _():
        for h in range(2):
            vbuf[h, pl.ds((row % 4) * piece, piece), :] = v_ref[:, h * lanes:(h + 1) * lanes]

    d_plane = ((row % 4) // 2) * 3
    d_self = v_self & (d_plane == z)
    d_copy = remote(d_ref, dbuf.at[pl.ds((row % 2) * piece, piece)], d_send, d_recv.at[row % 2], (d_plane, v_dev))

    @pl.when(d_self)
    def _():
        dbuf[pl.ds((row % 2) * piece, piece), :] = d_ref[...]

    for h in range(2):
        s_start(h)
    def x0_start(h):
        for m in range(4):
            x0_copy(h, m).start()

    def v_start(h):
        @pl.when(jnp.logical_not(v_self))
        def _():
            v_copy(h).start()

    x0_start(0)

    @pl.when(k == 0)
    def _():
        v_start(0)
        x0_start(1)

    @pl.when(k == 1)
    def _():
        x0_start(1)
        v_start(0)
    v_start(1)

    @pl.when(jnp.logical_not(d_self))
    def _():
        d_copy.start()

    def x0_forward(h):
        for m in range(3):
            x0_copy(h, m).wait_recv()
            x1_copy(h, m).start()

    def x0_finish(h):
        x0_copy(h, 3).wait_recv()
        for m in range(3):
            x1_copy(h, m).wait_recv()
        for m in range(4):
            x0_copy(h, m).wait_send()
        for m in range(3):
            x1_copy(h, m).wait_send()

    x0_forward(0)
    x0_finish(0)

    def index(step):
        n = step // PERIOD
        q = step % PERIOD
        valid = (step >= 0) & (n < PASSES) & (q < CHUNKS)
        return valid, n, q, n % 2, (n // 2) % 2

    def owner_is_reader(dirn):
        return (z == c) & (z == 3 * dirn)

    def slot(t, carry):
        def gather_copy(h, par, dirn, q, ring, m):
            rows = x_rows(h, 1 - par, k * block_rows + dirn * half + q * ch + c * sub, sub)
            return remote(rows, rows, g_send.at[ring, dirn, m], g_recv.at[h, dirn, q, m], (z, inplane[m]))

        def forward_copy(h, par, dirn, q, ring):
            rows = x_rows(h, 1 - par, k * block_rows + dirn * half + q * ch, ch)
            return remote(rows, rows, f_send.at[ring, dirn], f_recv.at[h, dirn, q], (z, partner))

        def forward(dirn):
            step = t - 3 * HOP - FORWARD
            old, n, q, h, par = index(step - RING)

            @pl.when(old & (n < PASSES - 2))
            def _():
                forward_copy(h, par, dirn, q, (step - RING) % RING).wait_send()
            valid, n, q, h, par = index(step)

            @pl.when(valid & (n < PASSES - 2))
            def _():
                for m in range(3):
                    gather_copy(h, par, dirn, q, step % RING, m).wait_recv()
                forward_copy(h, par, dirn, q, step % RING).start()

        def ready(dirn):
            step = t - 3 * HOP - READY
            valid, n, q, h, par = index(step)

            @pl.when(valid & (n < PASSES - 2))
            def _():
                forward_copy(h, par, dirn, q, step % RING).wait_recv()

        def gather(dirn):
            step = t - 3 * HOP - GATHER
            old, n, q, h, par = index(step - RING)

            @pl.when(old & (n < PASSES - 2))
            def _():
                for m in range(3):
                    gather_copy(h, par, dirn, q, (step - RING) % RING, m).wait_send()
            valid, n, q, h, par = index(step)

            @pl.when(valid & (n < PASSES - 2))
            def _():
                @pl.when(jnp.logical_not(owner_is_reader(dirn)))
                def _():
                    rows = x_rows(h, 1 - par, k * block_rows + dirn * half + q * ch + c * sub, sub)
                    remote(rows, rows, z_send.at[0, 0], z_recv.at[h, dirn, q], (z, row)).wait_recv()
                for m in range(3):
                    gather_copy(h, par, dirn, q, step % RING, m).start()

        def dangling_term():
            near = jnp.minimum(z, 3 - z)
            step = t - HOP * near
            valid, n, q, h, par = index(step)

            @pl.when(holds_v & valid & (q == 0))
            def _():
                def wait_one(src, carry):
                    sends = ((n < 2) | (src // 8 == 0) | (src // 8 == 3)) & (src != me)

                    @pl.when(sends)
                    def _():
                        remote(sstage.at[h], sbuf.at[h, src], s_send.at[h, 0], s_recv.at[h, src], (z, row)).wait_recv()
                    return carry
                lax.fori_loop(0, 32, wait_one, 0)

                ends = jnp.sum(sbuf[h, 0:8], axis=0) + jnp.sum(sbuf[h, 24:32], axis=0)
                coef[h] = ends

                @pl.when(n < 2)
                def _():
                    coef[h] += jnp.sum(sbuf[h, 8:24], axis=0)
                mass = jnp.sum(coef[h], axis=0, keepdims=True) / vertices
                coef[h] = jnp.broadcast_to(DAMPING * mass + (1.0 - DAMPING), (8, lanes))

        def reduce(dirn):
            pos = z if dirn == 1 else 3 - z
            after = z + 1 if dirn == 1 else z - 1
            owner = pos == 3

            def sum_copy(h, q, ring):
                return remote(sums.at[dirn, ring], rbuf.at[dirn, h, q], r_send.at[dirn, ring], r_recv.at[dirn, h, q],
                              (after, row))

            def out_place(h, q):
                rows = pl.ds((q % (CHUNKS // 2)) * ch, ch)
                return out_ref.at[rows, pl.ds(pl.multiple_of(h * lanes, lanes), lanes)]

            def out_row(q):
                return 4 * k + 2 * dirn + q // (CHUNKS // 2)

            def out_here(q):
                return (z == c) & (out_row(q) == row)

            def out_copy(h, q, ring):
                return remote(sums.at[dirn, ring], out_place(h, q), r_send.at[dirn, ring], o_recv.at[h, q % (CHUNKS // 2)],
                              (c, out_row(q)))

            def share_copy(h, par, q, ring, cc):
                rows = x_rows(h, 1 - par, k * block_rows + dirn * half + q * ch + cc * sub, sub)
                return remote(xs.at[ring, pl.ds(cc * sub, sub)], rows, z_send.at[ring, cc], z_recv.at[h, dirn, q],
                              (c, 2 * cc + k))

            step = t - HOP * pos
            old, n, q, h, par = index(step - RING)
            ring = (step - RING) % RING

            @pl.when(old & jnp.logical_not(owner))
            def _():
                sum_copy(h, q, ring).wait_send()

            @pl.when(old & owner & (n < PASSES - 2))
            def _():
                for cc in range(4):
                    @pl.when(jnp.logical_not((z == c) & (cc == c)))
                    def _():
                        share_copy(h, par, q, ring, cc).wait_send()

                @pl.when(q == CHUNKS - 1)
                def _():
                    s_wait_send(h)

            @pl.when(old & owner & (n >= PASSES - 2) & jnp.logical_not(out_here(q)))
            def _():
                out_copy(h, q, ring).wait_send()

            valid, n, q, h, par = index(step)
            ring = step % RING

            @pl.when(valid)
            def _():
                start = dirn * half + q * ch
                rows = pl.ds(start, ch)

                @pl.when(n == 0)
                def _():
                    a_copy(dirn, q).wait()
                prod = jnp.dot(a_v[rows, :], xbuf[h, par], preferred_element_type=jnp.float32)
                sums[dirn, ring] = prod * DAMPING

                part = 2 * dirn + q // (CHUNKS // 2)

                @pl.when(holds_v & (n < 2) & (q % (CHUNKS // 2) == 0) & (4 * k + part != row))
                def _():
                    place = vbuf.at[h, pl.ds(part * piece, piece)]
                    remote(place, place, v_send.at[0], v_recv.at[h, part], (z, row)).wait_recv()

                @pl.when(holds_v)
                def _():
                    sums[dirn, ring] += coef[h, 0:1, :] * vbuf[h, rows, :]

                @pl.when(pos > 0)
                def _():
                    sum_copy(h, q, ring).wait_recv()
                    sums[dirn, ring] += rbuf[dirn, h, q]

                @pl.when(jnp.logical_not(owner))
                def _():
                    sum_copy(h, q, ring).start()

                @pl.when(owner & (n < PASSES - 2))
                def _():
                    @pl.when((n == 0) & (q == 0))
                    def _():
                        for part in range(2):
                            @pl.when(jnp.logical_not((z == c) & (4 * k + 2 * dirn + part == row)))
                            def _():
                                place = dbuf.at[pl.ds(part * piece, piece)]
                                remote(d_ref, place, d_send, d_recv.at[part], (z, row)).wait_recv()
                    total = sums[dirn, ring]
                    low = total.astype(jnp.bfloat16)
                    xs[ring] = low
                    terms = dbuf[pl.ds(q * ch, ch), :].astype(jnp.float32) * total
                    mass = jnp.sum(terms.reshape(ch // 8, 8, lanes), axis=0)
                    for cc in range(4):
                        here = (z == c) & (cc == c)

                        @pl.when(here)
                        def _():
                            place = pl.ds(k * block_rows + start + cc * sub, sub)
                            xbuf[h, 1 - par, place, :] = low[cc * sub:(cc + 1) * sub]

                        @pl.when(jnp.logical_not(here))
                        def _():
                            share_copy(h, par, q, ring, cc).start()

                    @pl.when(q == 0)
                    def _():
                        sacc[...] = mass

                    @pl.when(q > 0)
                    def _():
                        sacc[...] += mass

                    @pl.when(q == CHUNKS - 1)
                    def _():
                        sstage[h] = sacc[...]
                        s_start(h)

                @pl.when(owner & (n >= PASSES - 2))
                def _():
                    @pl.when(out_here(q))
                    def _():
                        out_ref[pl.ds((q % (CHUNKS // 2)) * ch, ch), pl.ds(pl.multiple_of(h * lanes, lanes), lanes)] = sums[dirn, ring]

                    @pl.when(jnp.logical_not(out_here(q)))
                    def _():
                        out_copy(h, q, ring).start()

        @pl.when(t == PERIOD - 3)
        def _():
            x0_forward(1)

        @pl.when(t == PERIOD - 1)
        def _():
            x0_finish(1)
            for h in range(2):
                s_wait_send(h)

            @pl.when(jnp.logical_not(v_self))
            def _():
                for h in range(2):
                    v_copy(h).wait_send()

            @pl.when(jnp.logical_not(d_self))
            def _():
                d_copy.wait_send()

        for dirn in range(2):
            forward(dirn)
        for dirn in range(2):
            ready(dirn)
        dangling_term()
        reduce(1)
        for dirn in range(2):
            gather(dirn)
        reduce(0)
        return carry

    lax.fori_loop(0, PASSES * PERIOD + 3 * HOP + FORWARD + RING, slot, 0)

    made_here = (z == 3 * ((row % 4) // 2)) & (row == 2 * z + row // 4)

    @pl.when(jnp.logical_not(made_here))
    def _():
        for h in range(2):
            for q in range(CHUNKS // 2):
                place = out_ref.at[pl.ds(q * ch, ch), pl.ds(h * lanes, lanes)]
                remote(place, place, d_send, o_recv.at[h, q], (z, row)).wait_recv()


def solution(mesh):
    def local_sweeps(mat_tile, x_piece, tele_piece, dang_piece):
        block_rows, src = mat_tile.shape
        piece, vecs = x_piece.shape
        lanes = vecs // 2
        ch = block_rows // 2 // CHUNKS
        dang = jnp.broadcast_to(dang_piece.astype(jnp.bfloat16)[:, None], (piece, lanes))
        dma = pltpu.SemaphoreType.DMA
        return pl.pallas_call(
            functools.partial(kernel, block_rows, lanes),
            name='sweeps',
            out_shape=jax.ShapeDtypeStruct((piece, vecs), jnp.float32),
            in_specs=[pl.BlockSpec(memory_space=pltpu.HBM)] + [pl.BlockSpec(memory_space=pltpu.VMEM)] * 3,
            out_specs=pl.BlockSpec(memory_space=pltpu.VMEM),
            scratch_shapes=[
                pltpu.VMEM((block_rows, src), jnp.bfloat16),
                pltpu.VMEM((2, 2, src, lanes), jnp.bfloat16),
                pltpu.VMEM((2, 2, CHUNKS, ch, lanes), jnp.float32),
                pltpu.VMEM((2, RING, ch, lanes), jnp.float32),
                pltpu.VMEM((RING, ch, lanes), jnp.bfloat16),
                pltpu.VMEM((2, block_rows, lanes), jnp.float32),
                pltpu.VMEM((block_rows // 2, lanes), jnp.bfloat16),
                pltpu.VMEM((8, lanes), jnp.float32),
                pltpu.VMEM((2, 8, lanes), jnp.float32),
                pltpu.VMEM((2, 32, 8, lanes), jnp.float32),
                pltpu.VMEM((2, 8, lanes), jnp.float32),
                dma((2, CHUNKS)),
                dma((2, RING)),
                dma((2, 2, CHUNKS)),
                dma((RING, 4)),
                dma((2, 2, CHUNKS)),
                dma((RING, 2, 3)),
                dma((2, 2, CHUNKS, 3)),
                dma((RING, 2)),
                dma((2, 2, CHUNKS)),
                dma((2, 8)),
                dma((2, 32)),
                dma((2,)),
                dma((2, 4)),
                dma,
                dma((2,)),
                dma((2, 4)),
                dma((2, 4)),
                dma((2, 3)),
                dma((2, 3)),
                dma((2, CHUNKS // 2)),
            ],
            compiler_params=pltpu.CompilerParams(collective_id=0, has_side_effects=True,
                                                 vmem_limit_bytes=64 * 1024 * 1024 - 65536),
        )(mat_tile, x_piece, tele_piece, dang)

    vec_spec = P(('col', 'row'), None)
    return jax.shard_map(local_sweeps, mesh=mesh,
                         in_specs=(P('row', 'col'), vec_spec, vec_spec, P(('col', 'row'))),
                         out_specs=vec_spec, check_vma=False)
```

```python
import functools

import jax
import jax.numpy as jnp
from jax import lax
from jax.experimental import pallas as pl
from jax.experimental.pallas import tpu as pltpu
from jax.sharding import PartitionSpec as P

SWEEPS = 8
DAMPING = 0.85
MESH = pl.DeviceIdType.MESH

CHUNKS = 12
PERIOD = 12
HOP = 2
SPREAD = 3
GATHER = 5
FORWARD = 6
READY = 7
RING = 4
ORDER = 'GPWSUFD'
PASSES = 2 * SWEEPS


def kernel(block_rows, lanes, a_hbm, x_ref, v_ref, d_ref, out_ref,
           a_v, xbuf, rbuf, sums, xs, vbuf, dbuf, sacc, sstage, sbuf, coef,
           a_sem, r_send, r_recv, z_send, z_recv, g_send, g_recv, f_send, f_recv,
           s_send, s_recv, v_send, v_recv, d_send, d_recv, x0_send, x0_recv, x1_send, x1_recv, o_recv,
           tbuf, obuf, t_send, t_recv):
    z = lax.axis_index('col')
    row = lax.axis_index('row')
    k = row % 2
    x = (row // 2) % 2
    y = row // 4
    c = row // 2
    half = block_rows // 2
    ch = half // CHUNKS
    sub = ch // 4
    piece = block_rows // 4
    vertices = block_rows * 8
    inplane = (y * 4 + (1 - x) * 2 + k, (1 - y) * 4 + x * 2 + k, (1 - y) * 4 + (1 - x) * 2 + k)
    partner = c * 2 + (1 - k)

    def remote(src, dst, send, recv, dev):
        return pltpu.make_async_remote_copy(src_ref=src, dst_ref=dst, send_sem=send, recv_sem=recv,
                                            device_id=dev, device_id_type=MESH)

    def a_copy(dirn, q):
        rows = pl.ds(dirn * half + q * ch, ch)
        return pltpu.make_async_copy(a_hbm.at[rows], a_v.at[rows], a_sem.at[dirn, q])

    def start_a(q, carry):
        for dirn in range(2):
            a_copy(dirn, q).start()
        return carry
    lax.fori_loop(0, CHUNKS, start_a, 0)

    for h in range(2):
        xbuf[h, 0, pl.ds(row * piece, piece), :] = x_ref[:, h * lanes:(h + 1) * lanes].astype(jnp.bfloat16)
        terms = d_ref[...].astype(jnp.float32) * x_ref[:, h * lanes:(h + 1) * lanes]
        sstage[h] = jnp.sum(terms.reshape(piece // 8, 8, lanes), axis=0)

    barrier = pltpu.get_barrier_semaphore()
    me = z * 8 + row

    def greet(step, carry):
        other = (me + step) % 32
        pl.semaphore_signal(barrier, inc=1, device_id=(other // 8, other % 8), device_id_type=MESH)
        return carry
    lax.fori_loop(1, 32, greet, 0)
    pl.semaphore_wait(barrier, 31)

    def x_rows(h, par, start, size):
        return xbuf.at[h, par, pl.ds(start, size)]

    def x0_copy(h, m):
        dev = inplane[m] if m < 3 else partner
        mine = x_rows(h, 0, row * piece, piece)
        return remote(mine, mine, x0_send.at[h, m], x0_recv.at[h, m], (z, dev))

    def x1_copy(h, m):
        theirs = x_rows(h, 0, inplane[m] * piece, piece)
        return remote(theirs, theirs, x1_send.at[h, m], x1_recv.at[h, m], (z, partner))


    def s_copy(h, holder):
        dev = (holder // 2, (holder // 2) * 2 + holder % 2)
        return remote(sstage.at[h], sbuf.at[h, me], s_send.at[h, holder], s_recv.at[h, me], dev)

    holds_v = c == z

    def s_start(h):
        for holder in range(8):
            mine = (holder // 2 == z) & ((holder // 2) * 2 + holder % 2 == row)

            @pl.when(mine)
            def _():
                sbuf[h, me] = sstage[h]

            @pl.when(jnp.logical_not(mine))
            def _():
                s_copy(h, holder).start()

    def s_wait_send(h):
        for holder in range(8):
            @pl.when(jnp.logical_not((holder // 2 == z) & ((holder // 2) * 2 + holder % 2 == row)))
            def _():
                s_copy(h, holder).wait_send()


    v_dev = z * 2 + row // 4
    v_self = v_dev == row

    def v_copy(h, m):
        return remote(v_ref.at[pl.ds(m * ch, ch), pl.ds(pl.multiple_of(h * lanes, lanes), lanes)],
                      vbuf.at[h, pl.ds((row % 4) * piece + m * ch, ch)],
                      v_send.at[h, m], v_recv.at[h, row % 4, m], (z, v_dev))

    @pl.when(v_self)
    def _():
        for h in range(2):
            vbuf[h, pl.ds((row % 4) * piece, piece), :] = v_ref[:, h * lanes:(h + 1) * lanes]

    d_plane = ((row % 4) // 2) * 3
    d_self = v_self & (d_plane == z)
    d_copy = remote(d_ref, dbuf.at[pl.ds((row % 2) * piece, piece)], d_send, d_recv.at[row % 2], (d_plane, v_dev))

    @pl.when(d_self)
    def _():
        dbuf[pl.ds((row % 2) * piece, piece), :] = d_ref[...]

    for h in range(2):
        s_start(h)
    def x0_start(h):
        for m in range(4):
            x0_copy(h, m).start()

    x0_start(0)

    @pl.when(jnp.logical_not(d_self))
    def _():
        d_copy.start()

    @pl.when((k == 0) & jnp.logical_not(v_self))
    def _():
        for m in range(CHUNKS // 2):
            v_copy(0, m).start()
    x0_start(1)


    def x0_forward(h):
        for m in range(3):
            x0_copy(h, m).wait_recv()
            x1_copy(h, m).start()

    def x0_finish(h):
        x0_copy(h, 3).wait_recv()
        for m in range(3):
            x1_copy(h, m).wait_recv()
        for m in range(4):
            x0_copy(h, m).wait_send()
        for m in range(3):
            x1_copy(h, m).wait_send()

    x0_forward(0)
    x0_finish(0)

    def index(step):
        n = step // PERIOD
        q = step % PERIOD
        valid = (step >= 0) & (n < PASSES) & (q < CHUNKS)
        return valid, n, q, n % 2, (n // 2) % 2

    def owner_is_reader(dirn):
        return (z == c) & (z == 3 * dirn)

    def slot(t, carry):
        def gather_copy(h, par, dirn, q, ring, m):
            rows = x_rows(h, 1 - par, k * block_rows + dirn * half + q * ch + c * sub, sub)
            return remote(rows, rows, g_send.at[ring, dirn, m], g_recv.at[h, dirn, q, m], (z, inplane[m]))

        def forward_copy(h, par, dirn, q, ring):
            rows = x_rows(h, 1 - par, k * block_rows + dirn * half + q * ch, ch)
            return remote(rows, rows, f_send.at[ring, dirn], f_recv.at[h, dirn, q], (z, partner))

        def out_row(dirn, q):
            return 4 * k + 2 * dirn + q // (CHUNKS // 2)

        def out_place(h, q, cc):
            rows = pl.ds((q % (CHUNKS // 2)) * ch + cc * sub, sub)
            return out_ref.at[rows, pl.ds(pl.multiple_of(h * lanes, lanes), lanes)]

        def forward(dirn):
            step = t - 3 * HOP - FORWARD
            old, n, q, h, par = index(step - RING)

            @pl.when(old & (n < PASSES - 2))
            def _():
                forward_copy(h, par, dirn, q, (step - RING) % RING).wait_send()
            valid, n, q, h, par = index(step)

            @pl.when(valid & (n < PASSES - 2))
            def _():
                for m in range(3):
                    gather_copy(h, par, dirn, q, step % RING, m).wait_recv()
                forward_copy(h, par, dirn, q, step % RING).start()

        def ready(dirn):
            step = t - 3 * HOP - READY
            valid, n, q, h, par = index(step)

            @pl.when(valid & (n < PASSES - 2))
            def _():
                forward_copy(h, par, dirn, q, step % RING).wait_recv()

        def spread(dirn):
            def spread_copy(h, par, q, ring, src):
                rows = x_rows(h, 1 - par, k * block_rows + dirn * half + q * ch + c * sub, sub)
                return remote(tbuf.at[h, q, src], rows, t_send.at[ring, src], z_recv.at[h, dirn, q], (src, row))

            def result_copy(h, q, ring, src):
                return remote(obuf.at[h, q, src], out_place(h, q, c), t_send.at[ring, src],
                              o_recv.at[h, q % (CHUNKS // 2), c], (src, out_row(dirn, q)))

            step = t - 3 * HOP - SPREAD
            old, n, q, h, par = index(step - RING)
            at_end = z == 3 * dirn

            @pl.when(old & at_end & (n < PASSES - 2))
            def _():
                for src in range(4):
                    @pl.when((src != c) & (src != z))
                    def _():
                        spread_copy(h, par, q, (step - RING) % RING, src).wait_send()

            @pl.when(old & at_end & (n >= PASSES - 2))
            def _():
                for src in range(4):
                    @pl.when((src != c) & (src != z))
                    def _():
                        result_copy(h, q, (step - RING) % RING, src).wait_send()
            valid, n, q, h, par = index(step)

            @pl.when(valid & at_end & (n < PASSES - 2))
            def _():
                for src in range(4):
                    @pl.when((src != c) & (src != z))
                    def _():
                        remote(tbuf.at[h, q, src], tbuf.at[h, q, src], t_send.at[0, 0], t_recv.at[h, q, src],
                               (z, row)).wait_recv()
                        spread_copy(h, par, q, step % RING, src).start()

            @pl.when(valid & at_end & (n >= PASSES - 2))
            def _():
                for src in range(4):
                    @pl.when((src != c) & (src != z))
                    def _():
                        remote(obuf.at[h, q, src], obuf.at[h, q, src], t_send.at[0, 0], t_recv.at[h, q, src],
                               (z, row)).wait_recv()
                        result_copy(h, q, step % RING, src).start()

        def gather(dirn):
            step = t - 3 * HOP - GATHER
            old, n, q, h, par = index(step - RING)

            @pl.when(old & (n < PASSES - 2))
            def _():
                for m in range(3):
                    gather_copy(h, par, dirn, q, (step - RING) % RING, m).wait_send()
            valid, n, q, h, par = index(step)

            @pl.when(valid & (n < PASSES - 2))
            def _():
                @pl.when(jnp.logical_not(owner_is_reader(dirn)))
                def _():
                    rows = x_rows(h, 1 - par, k * block_rows + dirn * half + q * ch + c * sub, sub)
                    remote(rows, rows, z_send.at[0, 0], z_recv.at[h, dirn, q], (z, row)).wait_recv()
                for m in range(3):
                    gather_copy(h, par, dirn, q, step % RING, m).start()

        def dangling_term():
            near = jnp.minimum(z, 3 - z)
            step = t - HOP * near
            valid, n, q, h, par = index(step)

            @pl.when(holds_v & valid & (q == 0))
            def _():
                def wait_one(src, carry):
                    sends = ((n < 2) | (src // 8 == 0) | (src // 8 == 3)) & (src != me)

                    @pl.when(sends)
                    def _():
                        remote(sstage.at[h], sbuf.at[h, src], s_send.at[h, 0], s_recv.at[h, src], (z, row)).wait_recv()
                    return carry
                lax.fori_loop(0, 32, wait_one, 0)

                ends = jnp.sum(sbuf[h, 0:8], axis=0) + jnp.sum(sbuf[h, 24:32], axis=0)
                coef[h] = ends

                @pl.when(n < 2)
                def _():
                    coef[h] += jnp.sum(sbuf[h, 8:24], axis=0)
                mass = jnp.sum(coef[h], axis=0, keepdims=True) / vertices
                coef[h] = jnp.broadcast_to(DAMPING * mass + (1.0 - DAMPING), (8, lanes))

        def reduce(dirn):
            pos = z if dirn == 1 else 3 - z
            after = z + 1 if dirn == 1 else z - 1
            owner = pos == 3

            def sum_copy(h, q, ring):
                return remote(sums.at[dirn, ring], rbuf.at[dirn, h, q], r_send.at[dirn, ring], r_recv.at[dirn, h, q],
                              (after, row))

            def out_here(q):
                return (z == c) & (out_row(dirn, q) == row)

            def out_copies(h, q, ring, cc, act):
                mine = sums.at[dirn, ring, pl.ds(cc * sub, sub)]

                @pl.when(((cc == c) | (z == c)) & jnp.logical_not(out_here(q)))
                def _():
                    act(remote(mine, out_place(h, q, cc), z_send.at[ring, cc], o_recv.at[h, q % (CHUNKS // 2), cc],
                               (c, out_row(dirn, q))))

                @pl.when((cc != c) & (z != c))
                def _():
                    act(remote(mine, obuf.at[h, q, c], z_send.at[ring, cc], t_recv.at[h, q, c], (z, 2 * cc + k)))

            def share_rows(h, par, q, cc):
                return x_rows(h, 1 - par, k * block_rows + dirn * half + q * ch + cc * sub, sub)

            def share_copies(h, par, q, ring, cc, act):
                mine = xs.at[ring, pl.ds(cc * sub, sub)]

                @pl.when((cc == c) & (z != c))
                def _():
                    act(remote(mine, share_rows(h, par, q, cc), z_send.at[ring, cc], z_recv.at[h, dirn, q], (c, row)))

                @pl.when((cc != c) & (z == c))
                def _():
                    act(remote(mine, share_rows(h, par, q, cc), z_send.at[ring, cc], z_recv.at[h, dirn, q],
                               (z, 2 * cc + k)))

                @pl.when((cc != c) & (z != c))
                def _():
                    act(remote(mine, tbuf.at[h, q, c], z_send.at[ring, cc], t_recv.at[h, q, c], (z, 2 * cc + k)))

            step = t - HOP * pos
            old, n, q, h, par = index(step - RING)
            ring = (step - RING) % RING

            @pl.when(old & jnp.logical_not(owner))
            def _():
                sum_copy(h, q, ring).wait_send()

            @pl.when(old & owner & (n < PASSES - 2))
            def _():
                for cc in range(4):
                    share_copies(h, par, q, ring, cc, lambda copy: copy.wait_send())

                @pl.when(q == CHUNKS - 1)
                def _():
                    s_wait_send(h)

            @pl.when(old & owner & (n >= PASSES - 2))
            def _():
                for cc in range(4):
                    out_copies(h, q, ring, cc, lambda copy: copy.wait_send())

            valid, n, q, h, par = index(step)
            ring = step % RING

            @pl.when(valid)
            def _():
                start = dirn * half + q * ch
                rows = pl.ds(start, ch)

                @pl.when(n == 0)
                def _():
                    a_copy(dirn, q).wait()
                prod = jnp.dot(a_v[rows, :], xbuf[h, par], preferred_element_type=jnp.float32)
                sums[dirn, ring] = prod * DAMPING

                part = 2 * dirn + q // (CHUNKS // 2)

                @pl.when(holds_v & (n < 2) & (4 * k + part != row))
                def _():
                    place = vbuf.at[h, rows]
                    remote(place, place, v_send.at[0, 0], v_recv.at[h, part, q % (CHUNKS // 2)], (z, row)).wait_recv()

                @pl.when(holds_v)
                def _():
                    sums[dirn, ring] += coef[h, 0:1, :] * vbuf[h, rows, :]

                @pl.when(pos > 0)
                def _():
                    sum_copy(h, q, ring).wait_recv()
                    sums[dirn, ring] += rbuf[dirn, h, q]

                @pl.when(jnp.logical_not(owner))
                def _():
                    sum_copy(h, q, ring).start()

                @pl.when(owner & (n < PASSES - 2))
                def _():
                    @pl.when((n == 0) & (q == 0))
                    def _():
                        for part in range(2):
                            @pl.when(jnp.logical_not((z == c) & (4 * k + 2 * dirn + part == row)))
                            def _():
                                place = dbuf.at[pl.ds(part * piece, piece)]
                                remote(d_ref, place, d_send, d_recv.at[part], (z, row)).wait_recv()
                    total = sums[dirn, ring]
                    low = total.astype(jnp.bfloat16)
                    xs[ring] = low
                    terms = dbuf[pl.ds(q * ch, ch), :].astype(jnp.float32) * total
                    mass = jnp.sum(terms.reshape(ch // 8, 8, lanes), axis=0)
                    for cc in range(4):
                        here = (z == c) & (cc == c)

                        @pl.when(here)
                        def _():
                            place = pl.ds(k * block_rows + start + cc * sub, sub)
                            xbuf[h, 1 - par, place, :] = low[cc * sub:(cc + 1) * sub]

                        share_copies(h, par, q, ring, cc, lambda copy: copy.start())

                    @pl.when(q == 0)
                    def _():
                        sacc[...] = mass

                    @pl.when(q > 0)
                    def _():
                        sacc[...] += mass

                    @pl.when(q == CHUNKS - 1)
                    def _():
                        sstage[h] = sacc[...]
                        s_start(h)

                @pl.when(owner & (n >= PASSES - 2))
                def _():
                    @pl.when(out_here(q))
                    def _():
                        out_ref[pl.ds((q % (CHUNKS // 2)) * ch, ch), pl.ds(pl.multiple_of(h * lanes, lanes), lanes)] = sums[dirn, ring]

                    for cc in range(4):
                        out_copies(h, q, ring, cc, lambda copy: copy.start())

        @pl.when(t == PERIOD - 3)
        def _():
            x0_forward(1)

        @pl.when(t == PERIOD - 1)
        def _():
            x0_finish(1)
            for h in range(2):
                s_wait_send(h)


            @pl.when(jnp.logical_not(d_self))
            def _():
                d_copy.wait_send()

        turn = t + (1 - k) * (CHUNKS // 2)
        turn_h = turn // PERIOD
        turn_m = turn % PERIOD

        @pl.when((turn < 2 * PERIOD) & (turn_m < CHUNKS // 2) & jnp.logical_not(v_self))
        def _():
            v_copy(turn_h, turn_m).start()

        @pl.when((t == 2 * PERIOD) & jnp.logical_not(v_self))
        def _():
            for h in range(2):
                for m in range(CHUNKS // 2):
                    v_copy(h, m).wait_send()

        def both(stage):
            for dirn in range(2):
                stage(dirn)
        stages = {'F': lambda: both(forward), 'W': lambda: both(ready), 'S': dangling_term, 'U': lambda: reduce(1),
                  'G': lambda: both(gather), 'P': lambda: both(spread), 'D': lambda: reduce(0)}
        for name in ORDER:
            stages[name]()
        return carry

    lax.fori_loop(0, PASSES * PERIOD + 3 * HOP + FORWARD + RING, slot, 0)

    made_here = (z == 3 * ((row % 4) // 2)) & (row == 2 * z + row // 4)

    @pl.when(jnp.logical_not(made_here))
    def _():
        for h in range(2):
            for q in range(CHUNKS // 2):
                for cc in range(4):
                    place = out_ref.at[pl.ds(q * ch + cc * sub, sub), pl.ds(h * lanes, lanes)]
                    remote(place, place, d_send, o_recv.at[h, q, cc], (z, row)).wait_recv()


def solution(mesh):
    def local_sweeps(mat_tile, x_piece, tele_piece, dang_piece):
        block_rows, src = mat_tile.shape
        piece, vecs = x_piece.shape
        lanes = vecs // 2
        ch = block_rows // 2 // CHUNKS
        dang = jnp.broadcast_to(dang_piece.astype(jnp.bfloat16)[:, None], (piece, lanes))
        dma = pltpu.SemaphoreType.DMA
        return pl.pallas_call(
            functools.partial(kernel, block_rows, lanes),
            name='sweeps',
            out_shape=jax.ShapeDtypeStruct((piece, vecs), jnp.float32),
            in_specs=[pl.BlockSpec(memory_space=pltpu.HBM)] + [pl.BlockSpec(memory_space=pltpu.VMEM)] * 3,
            out_specs=pl.BlockSpec(memory_space=pltpu.VMEM),
            scratch_shapes=[
                pltpu.VMEM((block_rows, src), jnp.bfloat16),
                pltpu.VMEM((2, 2, src, lanes), jnp.bfloat16),
                pltpu.VMEM((2, 2, CHUNKS, ch, lanes), jnp.float32),
                pltpu.VMEM((2, RING, ch, lanes), jnp.float32),
                pltpu.VMEM((RING, ch, lanes), jnp.bfloat16),
                pltpu.VMEM((2, block_rows, lanes), jnp.float32),
                pltpu.VMEM((block_rows // 2, lanes), jnp.bfloat16),
                pltpu.VMEM((8, lanes), jnp.float32),
                pltpu.VMEM((2, 8, lanes), jnp.float32),
                pltpu.VMEM((2, 32, 8, lanes), jnp.float32),
                pltpu.VMEM((2, 8, lanes), jnp.float32),
                dma((2, CHUNKS)),
                dma((2, RING)),
                dma((2, 2, CHUNKS)),
                dma((RING, 4)),
                dma((2, 2, CHUNKS)),
                dma((RING, 2, 3)),
                dma((2, 2, CHUNKS, 3)),
                dma((RING, 2)),
                dma((2, 2, CHUNKS)),
                dma((2, 8)),
                dma((2, 32)),
                dma((2, CHUNKS // 2)),
                dma((2, 4, CHUNKS // 2)),
                dma,
                dma((2,)),
                dma((2, 4)),
                dma((2, 4)),
                dma((2, 3)),
                dma((2, 3)),
                dma((2, CHUNKS // 2, 4)),
                pltpu.VMEM((2, CHUNKS, 4, ch // 4, lanes), jnp.bfloat16),
                pltpu.VMEM((2, CHUNKS, 4, ch // 4, lanes), jnp.float32),
                dma((RING, 4)),
                dma((2, CHUNKS, 4)),
            ],
            compiler_params=pltpu.CompilerParams(collective_id=0, has_side_effects=True,
                                                 vmem_limit_bytes=64 * 1024 * 1024 - 65536),
        )(mat_tile, x_piece, tele_piece, dang)

    vec_spec = P(('col', 'row'), None)
    return jax.shard_map(local_sweeps, mesh=mesh,
                         in_specs=(P('row', 'col'), vec_spec, vec_spec, P(('col', 'row'))),
                         out_specs=vec_spec, check_vma=False)
```

```python
import functools

import jax
import jax.numpy as jnp
from jax import lax
from jax.experimental import pallas as pl
from jax.experimental.pallas import tpu as pltpu
from jax.sharding import PartitionSpec as P

SWEEPS = 8
DAMPING = 0.85
MESH = pl.DeviceIdType.MESH

CHUNKS = 12
PERIOD = 12
HOP = 2
SPREAD = 3
GATHER = 5
FORWARD = 6
READY = 7
RING = 4
RELAY = 3
ORDER = 'GPWSUFD'
PASSES = 2 * SWEEPS


def kernel(block_rows, lanes, a_hbm, x_ref, v_ref, d_ref, out_ref,
           a_v, xbuf, rbuf, sums, xs, vbuf, dbuf, sacc, sstage, sbuf, coef,
           a_sem, r_send, r_recv, z_send, z_recv, g_send, g_recv, f_send, f_recv,
           s_send, s_recv, v_send, v_recv, d_send, d_recv, x0_send, x0_recv, x1_send, x1_recv, o_recv,
           tbuf, obuf, t_send, t_recv, vstage, w_send, w_recv):
    z = lax.axis_index('col')
    row = lax.axis_index('row')
    k = row % 2
    x = (row // 2) % 2
    y = row // 4
    c = row // 2
    half = block_rows // 2
    ch = half // CHUNKS
    sub = ch // 4
    piece = block_rows // 4
    vertices = block_rows * 8
    inplane = (y * 4 + (1 - x) * 2 + k, (1 - y) * 4 + x * 2 + k, (1 - y) * 4 + (1 - x) * 2 + k)
    partner = c * 2 + (1 - k)

    def remote(src, dst, send, recv, dev):
        return pltpu.make_async_remote_copy(src_ref=src, dst_ref=dst, send_sem=send, recv_sem=recv,
                                            device_id=dev, device_id_type=MESH)

    def a_copy(dirn, q):
        rows = pl.ds(dirn * half + q * ch, ch)
        return pltpu.make_async_copy(a_hbm.at[rows], a_v.at[rows], a_sem.at[dirn, q])

    def start_a(q, carry):
        for dirn in range(2):
            a_copy(dirn, q).start()
        return carry
    lax.fori_loop(0, CHUNKS, start_a, 0)

    for h in range(2):
        xbuf[h, 0, pl.ds(row * piece, piece), :] = x_ref[:, h * lanes:(h + 1) * lanes].astype(jnp.bfloat16)
        terms = d_ref[...].astype(jnp.float32) * x_ref[:, h * lanes:(h + 1) * lanes]
        sstage[h] = jnp.sum(terms.reshape(piece // 8, 8, lanes), axis=0)

    barrier = pltpu.get_barrier_semaphore()
    me = z * 8 + row

    def greet(step, carry):
        other = (me + step) % 32
        pl.semaphore_signal(barrier, inc=1, device_id=(other // 8, other % 8), device_id_type=MESH)
        return carry
    lax.fori_loop(1, 32, greet, 0)
    pl.semaphore_wait(barrier, 31)

    def x_rows(h, par, start, size):
        return xbuf.at[h, par, pl.ds(start, size)]

    def x0_copy(h, m):
        dev = inplane[m] if m < 3 else partner
        mine = x_rows(h, 0, row * piece, piece)
        return remote(mine, mine, x0_send.at[h, m], x0_recv.at[h, m], (z, dev))

    def x1_copy(h, m):
        theirs = x_rows(h, 0, inplane[m] * piece, piece)
        return remote(theirs, theirs, x1_send.at[h, m], x1_recv.at[h, m], (z, partner))


    def s_copy(h, holder):
        dev = (holder // 2, (holder // 2) * 2 + holder % 2)
        return remote(sstage.at[h], sbuf.at[h, me], s_send.at[h, holder], s_recv.at[h, me], dev)

    holds_v = c == z

    def s_start(h):
        for holder in range(8):
            mine = (holder // 2 == z) & ((holder // 2) * 2 + holder % 2 == row)

            @pl.when(mine)
            def _():
                sbuf[h, me] = sstage[h]

            @pl.when(jnp.logical_not(mine))
            def _():
                s_copy(h, holder).start()

    def s_wait_send(h):
        for holder in range(8):
            @pl.when(jnp.logical_not((holder // 2 == z) & ((holder // 2) * 2 + holder % 2 == row)))
            def _():
                s_copy(h, holder).wait_send()


    v_dev = z * 2 + row // 4
    v_self = v_dev == row

    def v_copy(h, m):
        return remote(v_ref.at[pl.ds(m * ch, ch), pl.ds(pl.multiple_of(h * lanes, lanes), lanes)],
                      vbuf.at[h, pl.ds((row % 4) * piece + m * ch, ch)],
                      v_send.at[h, m], v_recv.at[h, row % 4, m], (z, v_dev))

    far_row = 2 * (3 - z) + 1
    near_row = 2 * ((z // 2) * 2 + 1 - z % 2) + 1
    is_far = row == far_row
    is_relay = row == near_row

    def far_copy(h, m):
        return remote(v_ref.at[pl.ds(m * ch, ch), pl.ds(pl.multiple_of(h * lanes, lanes), lanes)],
                      vstage.at[h, pl.ds(m * ch, ch)], v_send.at[h, m], w_recv.at[h, m], (z, near_row))

    def relay_copy(h, m):
        return remote(vstage.at[h, pl.ds(m * ch, ch)], vbuf.at[h, pl.ds((far_row % 4) * piece + m * ch, ch)],
                      w_send.at[h, m], v_recv.at[h, far_row % 4, m], (z, z * 2 + far_row // 4))

    @pl.when(v_self)
    def _():
        for h in range(2):
            vbuf[h, pl.ds((row % 4) * piece, piece), :] = v_ref[:, h * lanes:(h + 1) * lanes]

    d_plane = ((row % 4) // 2) * 3
    d_self = v_self & (d_plane == z)
    d_copy = remote(d_ref, dbuf.at[pl.ds((row % 2) * piece, piece)], d_send, d_recv.at[row % 2], (d_plane, v_dev))

    @pl.when(d_self)
    def _():
        dbuf[pl.ds((row % 2) * piece, piece), :] = d_ref[...]

    for h in range(2):
        s_start(h)
    def x0_start(h):
        for m in range(4):
            x0_copy(h, m).start()

    x0_start(0)

    @pl.when(jnp.logical_not(d_self))
    def _():
        d_copy.start()

    @pl.when((k == 0) & jnp.logical_not(v_self))
    def _():
        for m in range(CHUNKS // 2):
            v_copy(0, m).start()
    x0_start(1)


    def x0_forward(h):
        for m in range(3):
            x0_copy(h, m).wait_recv()
            x1_copy(h, m).start()

    def x0_finish(h):
        x0_copy(h, 3).wait_recv()
        for m in range(3):
            x1_copy(h, m).wait_recv()
        for m in range(4):
            x0_copy(h, m).wait_send()
        for m in range(3):
            x1_copy(h, m).wait_send()

    x0_forward(0)
    x0_finish(0)

    def index(step):
        n = step // PERIOD
        q = step % PERIOD
        valid = (step >= 0) & (n < PASSES) & (q < CHUNKS)
        return valid, n, q, n % 2, (n // 2) % 2

    def owner_is_reader(dirn):
        return (z == c) & (z == 3 * dirn)

    def slot(t, carry):
        def gather_copy(h, par, dirn, q, ring, m):
            rows = x_rows(h, 1 - par, k * block_rows + dirn * half + q * ch + c * sub, sub)
            return remote(rows, rows, g_send.at[ring, dirn, m], g_recv.at[h, dirn, q, m], (z, inplane[m]))

        def forward_copy(h, par, dirn, q, ring):
            rows = x_rows(h, 1 - par, k * block_rows + dirn * half + q * ch, ch)
            return remote(rows, rows, f_send.at[ring, dirn], f_recv.at[h, dirn, q], (z, partner))

        def out_row(dirn, q):
            return 4 * k + 2 * dirn + q // (CHUNKS // 2)

        def out_place(h, q, cc):
            rows = pl.ds((q % (CHUNKS // 2)) * ch + cc * sub, sub)
            return out_ref.at[rows, pl.ds(pl.multiple_of(h * lanes, lanes), lanes)]

        def forward(dirn):
            step = t - 3 * HOP - FORWARD
            old, n, q, h, par = index(step - RING)

            @pl.when(old & (n < PASSES - 2))
            def _():
                forward_copy(h, par, dirn, q, (step - RING) % RING).wait_send()
            valid, n, q, h, par = index(step)

            @pl.when(valid & (n < PASSES - 2))
            def _():
                for m in range(3):
                    gather_copy(h, par, dirn, q, step % RING, m).wait_recv()
                forward_copy(h, par, dirn, q, step % RING).start()

        def ready(dirn):
            step = t - 3 * HOP - READY
            valid, n, q, h, par = index(step)

            @pl.when(valid & (n < PASSES - 2))
            def _():
                forward_copy(h, par, dirn, q, step % RING).wait_recv()

        def spread(dirn):
            def spread_copy(h, par, q, ring, src):
                rows = x_rows(h, 1 - par, k * block_rows + dirn * half + q * ch + c * sub, sub)
                return remote(tbuf.at[h, q, src], rows, t_send.at[ring, src], z_recv.at[h, dirn, q], (src, row))

            def result_copy(h, q, ring, src):
                return remote(obuf.at[h, q, src], out_place(h, q, c), t_send.at[ring, src],
                              o_recv.at[h, q % (CHUNKS // 2), c], (src, out_row(dirn, q)))

            step = t - 3 * HOP - SPREAD
            old, n, q, h, par = index(step - RING)
            at_end = z == 3 * dirn

            @pl.when(old & at_end & (n < PASSES - 2))
            def _():
                for src in range(4):
                    @pl.when((src != c) & (src != z))
                    def _():
                        spread_copy(h, par, q, (step - RING) % RING, src).wait_send()

            @pl.when(old & at_end & (n >= PASSES - 2))
            def _():
                for src in range(4):
                    @pl.when((src != c) & (src != z))
                    def _():
                        result_copy(h, q, (step - RING) % RING, src).wait_send()
            valid, n, q, h, par = index(step)

            @pl.when(valid & at_end & (n < PASSES - 2))
            def _():
                for src in range(4):
                    @pl.when((src != c) & (src != z))
                    def _():
                        remote(tbuf.at[h, q, src], tbuf.at[h, q, src], t_send.at[0, 0], t_recv.at[h, q, src],
                               (z, row)).wait_recv()
                        spread_copy(h, par, q, step % RING, src).start()

            @pl.when(valid & at_end & (n >= PASSES - 2))
            def _():
                for src in range(4):
                    @pl.when((src != c) & (src != z))
                    def _():
                        remote(obuf.at[h, q, src], obuf.at[h, q, src], t_send.at[0, 0], t_recv.at[h, q, src],
                               (z, row)).wait_recv()
                        result_copy(h, q, step % RING, src).start()

        def gather(dirn):
            step = t - 3 * HOP - GATHER
            old, n, q, h, par = index(step - RING)

            @pl.when(old & (n < PASSES - 2))
            def _():
                for m in range(3):
                    gather_copy(h, par, dirn, q, (step - RING) % RING, m).wait_send()
            valid, n, q, h, par = index(step)

            @pl.when(valid & (n < PASSES - 2))
            def _():
                @pl.when(jnp.logical_not(owner_is_reader(dirn)))
                def _():
                    rows = x_rows(h, 1 - par, k * block_rows + dirn * half + q * ch + c * sub, sub)
                    remote(rows, rows, z_send.at[0, 0], z_recv.at[h, dirn, q], (z, row)).wait_recv()
                for m in range(3):
                    gather_copy(h, par, dirn, q, step % RING, m).start()

        def dangling_term():
            near = jnp.minimum(z, 3 - z)
            step = t - HOP * near
            valid, n, q, h, par = index(step)

            @pl.when(holds_v & valid & (q == 0))
            def _():
                def wait_one(src, carry):
                    sends = ((n < 2) | (src // 8 == 0) | (src // 8 == 3)) & (src != me)

                    @pl.when(sends)
                    def _():
                        remote(sstage.at[h], sbuf.at[h, src], s_send.at[h, 0], s_recv.at[h, src], (z, row)).wait_recv()
                    return carry
                lax.fori_loop(0, 32, wait_one, 0)

                ends = jnp.sum(sbuf[h, 0:8], axis=0) + jnp.sum(sbuf[h, 24:32], axis=0)
                coef[h] = ends

                @pl.when(n < 2)
                def _():
                    coef[h] += jnp.sum(sbuf[h, 8:24], axis=0)
                mass = jnp.sum(coef[h], axis=0, keepdims=True) / vertices
                coef[h] = jnp.broadcast_to(DAMPING * mass + (1.0 - DAMPING), (8, lanes))

        def reduce(dirn):
            pos = z if dirn == 1 else 3 - z
            after = z + 1 if dirn == 1 else z - 1
            owner = pos == 3

            def sum_copy(h, q, ring):
                return remote(sums.at[dirn, ring], rbuf.at[dirn, h, q], r_send.at[dirn, ring], r_recv.at[dirn, h, q],
                              (after, row))

            def out_here(q):
                return (z == c) & (out_row(dirn, q) == row)

            def out_copies(h, q, ring, cc, act):
                mine = sums.at[dirn, ring, pl.ds(cc * sub, sub)]

                @pl.when(((cc == c) | (z == c)) & jnp.logical_not(out_here(q)))
                def _():
                    act(remote(mine, out_place(h, q, cc), z_send.at[ring, cc], o_recv.at[h, q % (CHUNKS // 2), cc],
                               (c, out_row(dirn, q))))

                @pl.when((cc != c) & (z != c))
                def _():
                    act(remote(mine, obuf.at[h, q, c], z_send.at[ring, cc], t_recv.at[h, q, c], (z, 2 * cc + k)))

            def share_rows(h, par, q, cc):
                return x_rows(h, 1 - par, k * block_rows + dirn * half + q * ch + cc * sub, sub)

            def share_copies(h, par, q, ring, cc, act):
                mine = xs.at[ring, pl.ds(cc * sub, sub)]

                @pl.when((cc == c) & (z != c))
                def _():
                    act(remote(mine, share_rows(h, par, q, cc), z_send.at[ring, cc], z_recv.at[h, dirn, q], (c, row)))

                @pl.when((cc != c) & (z == c))
                def _():
                    act(remote(mine, share_rows(h, par, q, cc), z_send.at[ring, cc], z_recv.at[h, dirn, q],
                               (z, 2 * cc + k)))

                @pl.when((cc != c) & (z != c))
                def _():
                    act(remote(mine, tbuf.at[h, q, c], z_send.at[ring, cc], t_recv.at[h, q, c], (z, 2 * cc + k)))

            step = t - HOP * pos
            old, n, q, h, par = index(step - RING)
            ring = (step - RING) % RING

            @pl.when(old & jnp.logical_not(owner))
            def _():
                sum_copy(h, q, ring).wait_send()

            @pl.when(old & owner & (n < PASSES - 2))
            def _():
                for cc in range(4):
                    share_copies(h, par, q, ring, cc, lambda copy: copy.wait_send())

                @pl.when(q == CHUNKS - 1)
                def _():
                    s_wait_send(h)

            @pl.when(old & owner & (n >= PASSES - 2))
            def _():
                for cc in range(4):
                    out_copies(h, q, ring, cc, lambda copy: copy.wait_send())

            valid, n, q, h, par = index(step)
            ring = step % RING

            @pl.when(valid)
            def _():
                start = dirn * half + q * ch
                rows = pl.ds(start, ch)

                @pl.when(n == 0)
                def _():
                    a_copy(dirn, q).wait()
                prod = jnp.dot(a_v[rows, :], xbuf[h, par], preferred_element_type=jnp.float32)
                sums[dirn, ring] = prod * DAMPING

                part = 2 * dirn + q // (CHUNKS // 2)

                @pl.when(holds_v & (n < 2) & (4 * k + part != row))
                def _():
                    place = vbuf.at[h, rows]
                    remote(place, place, v_send.at[0, 0], v_recv.at[h, part, q % (CHUNKS // 2)], (z, row)).wait_recv()

                @pl.when(holds_v)
                def _():
                    sums[dirn, ring] += coef[h, 0:1, :] * vbuf[h, rows, :]

                @pl.when(pos > 0)
                def _():
                    sum_copy(h, q, ring).wait_recv()
                    sums[dirn, ring] += rbuf[dirn, h, q]

                @pl.when(jnp.logical_not(owner))
                def _():
                    sum_copy(h, q, ring).start()

                @pl.when(owner & (n < PASSES - 2))
                def _():
                    @pl.when((n == 0) & (q == 0))
                    def _():
                        for part in range(2):
                            @pl.when(jnp.logical_not((z == c) & (4 * k + 2 * dirn + part == row)))
                            def _():
                                place = dbuf.at[pl.ds(part * piece, piece)]
                                remote(d_ref, place, d_send, d_recv.at[part], (z, row)).wait_recv()
                    total = sums[dirn, ring]
                    low = total.astype(jnp.bfloat16)
                    xs[ring] = low
                    terms = dbuf[pl.ds(q * ch, ch), :].astype(jnp.float32) * total
                    mass = jnp.sum(terms.reshape(ch // 8, 8, lanes), axis=0)
                    for cc in range(4):
                        here = (z == c) & (cc == c)

                        @pl.when(here)
                        def _():
                            place = pl.ds(k * block_rows + start + cc * sub, sub)
                            xbuf[h, 1 - par, place, :] = low[cc * sub:(cc + 1) * sub]

                        share_copies(h, par, q, ring, cc, lambda copy: copy.start())

                    @pl.when(q == 0)
                    def _():
                        sacc[...] = mass

                    @pl.when(q > 0)
                    def _():
                        sacc[...] += mass

                    @pl.when(q == CHUNKS - 1)
                    def _():
                        sstage[h] = sacc[...]
                        s_start(h)

                @pl.when(owner & (n >= PASSES - 2))
                def _():
                    @pl.when(out_here(q))
                    def _():
                        out_ref[pl.ds((q % (CHUNKS // 2)) * ch, ch), pl.ds(pl.multiple_of(h * lanes, lanes), lanes)] = sums[dirn, ring]

                    for cc in range(4):
                        out_copies(h, q, ring, cc, lambda copy: copy.start())

        @pl.when(t == PERIOD - 3)
        def _():
            x0_forward(1)

        @pl.when(t == PERIOD - 1)
        def _():
            x0_finish(1)
            for h in range(2):
                s_wait_send(h)


            @pl.when(jnp.logical_not(d_self))
            def _():
                d_copy.wait_send()

        turn = t + (1 - k) * (CHUNKS // 2)
        turn_h = turn // PERIOD
        turn_m = turn % PERIOD

        sends_v = (turn < 2 * PERIOD) & (turn_m < CHUNKS // 2) & jnp.logical_not(v_self)

        @pl.when(sends_v & jnp.logical_not(is_far))
        def _():
            v_copy(turn_h, turn_m).start()

        @pl.when(sends_v & is_far)
        def _():
            far_copy(turn_h, turn_m).start()

        past = t - RELAY

        @pl.when((past >= 0) & (past < 2 * PERIOD) & (past % PERIOD < CHUNKS // 2) & is_relay)
        def _():
            far_copy(past // PERIOD, past % PERIOD).wait_recv()
            relay_copy(past // PERIOD, past % PERIOD).start()

        @pl.when((t == 2 * PERIOD) & jnp.logical_not(v_self))
        def _():
            for h in range(2):
                for m in range(CHUNKS // 2):
                    v_copy(h, m).wait_send()

        @pl.when((t == 2 * PERIOD) & is_relay)
        def _():
            for h in range(2):
                for m in range(CHUNKS // 2):
                    relay_copy(h, m).wait_send()

        def both(stage):
            for dirn in range(2):
                stage(dirn)
        stages = {'F': lambda: both(forward), 'W': lambda: both(ready), 'S': dangling_term, 'U': lambda: reduce(1),
                  'G': lambda: both(gather), 'P': lambda: both(spread), 'D': lambda: reduce(0)}
        for name in ORDER:
            stages[name]()
        return carry

    lax.fori_loop(0, PASSES * PERIOD + 3 * HOP + FORWARD + RING, slot, 0)

    made_here = (z == 3 * ((row % 4) // 2)) & (row == 2 * z + row // 4)

    @pl.when(jnp.logical_not(made_here))
    def _():
        for h in range(2):
            for q in range(CHUNKS // 2):
                for cc in range(4):
                    place = out_ref.at[pl.ds(q * ch + cc * sub, sub), pl.ds(h * lanes, lanes)]
                    remote(place, place, d_send, o_recv.at[h, q, cc], (z, row)).wait_recv()


def solution(mesh):
    def local_sweeps(mat_tile, x_piece, tele_piece, dang_piece):
        block_rows, src = mat_tile.shape
        piece, vecs = x_piece.shape
        lanes = vecs // 2
        ch = block_rows // 2 // CHUNKS
        dang = jnp.broadcast_to(dang_piece.astype(jnp.bfloat16)[:, None], (piece, lanes))
        dma = pltpu.SemaphoreType.DMA
        return pl.pallas_call(
            functools.partial(kernel, block_rows, lanes),
            name='sweeps',
            out_shape=jax.ShapeDtypeStruct((piece, vecs), jnp.float32),
            in_specs=[pl.BlockSpec(memory_space=pltpu.HBM)] + [pl.BlockSpec(memory_space=pltpu.VMEM)] * 3,
            out_specs=pl.BlockSpec(memory_space=pltpu.VMEM),
            scratch_shapes=[
                pltpu.VMEM((block_rows, src), jnp.bfloat16),
                pltpu.VMEM((2, 2, src, lanes), jnp.bfloat16),
                pltpu.VMEM((2, 2, CHUNKS, ch, lanes), jnp.float32),
                pltpu.VMEM((2, RING, ch, lanes), jnp.float32),
                pltpu.VMEM((RING, ch, lanes), jnp.bfloat16),
                pltpu.VMEM((2, block_rows, lanes), jnp.float32),
                pltpu.VMEM((block_rows // 2, lanes), jnp.bfloat16),
                pltpu.VMEM((8, lanes), jnp.float32),
                pltpu.VMEM((2, 8, lanes), jnp.float32),
                pltpu.VMEM((2, 32, 8, lanes), jnp.float32),
                pltpu.VMEM((2, 8, lanes), jnp.float32),
                dma((2, CHUNKS)),
                dma((2, RING)),
                dma((2, 2, CHUNKS)),
                dma((RING, 4)),
                dma((2, 2, CHUNKS)),
                dma((RING, 2, 3)),
                dma((2, 2, CHUNKS, 3)),
                dma((RING, 2)),
                dma((2, 2, CHUNKS)),
                dma((2, 8)),
                dma((2, 32)),
                dma((2, CHUNKS // 2)),
                dma((2, 4, CHUNKS // 2)),
                dma,
                dma((2,)),
                dma((2, 4)),
                dma((2, 4)),
                dma((2, 3)),
                dma((2, 3)),
                dma((2, CHUNKS // 2, 4)),
                pltpu.VMEM((2, CHUNKS, 4, ch // 4, lanes), jnp.bfloat16),
                pltpu.VMEM((2, CHUNKS, 4, ch // 4, lanes), jnp.float32),
                dma((RING, 4)),
                dma((2, CHUNKS, 4)),
                pltpu.VMEM((2, piece, lanes), jnp.float32),
                dma((2, CHUNKS // 2)),
                dma((2, CHUNKS // 2)),
            ],
            compiler_params=pltpu.CompilerParams(collective_id=0, has_side_effects=True,
                                                 vmem_limit_bytes=64 * 1024 * 1024 - 65536),
        )(mat_tile, x_piece, tele_piece, dang)

    vec_spec = P(('col', 'row'), None)
    return jax.shard_map(local_sweeps, mesh=mesh,
                         in_specs=(P('row', 'col'), vec_spec, vec_spec, P(('col', 'row'))),
                         out_specs=vec_spec, check_vma=False)
```
